128 devices in a mesh: tp: 2 (over core), dp: 64 (over z, y, x).
Axes of the slice: x: 4, y: 4, z: 4, core: 2. Of those that a mesh axis runs over, the one named last changes fastest.
Arguments:
- hidden: bfloat16 [64, 1024, 512], P('dp')
- labels: int32 [64, 1024], P('dp')
- loss_mask: int32 [64, 1024], P('dp')
- ln_gain: float32 [512], replicated
- ln_bias: float32 [512], replicated
- w_query: bfloat16 [512, 8, 64], P(None, 'tp')
- w_key: bfloat16 [512, 8, 64], P(None, 'tp')
- w_value: bfloat16 [512, 8, 64], P(None, 'tp')
- w_attn_out: bfloat16 [8, 64, 512], P('tp')
- w_fc_in: bfloat16 [512, 2048], P(None, 'tp')
- b_fc_in: float32 [2048], P('tp')
- w_fc_out: bfloat16 [2048, 512], P('tp')
- b_fc_out: float32 [512], replicated
- lnf_gain: float32 [512], replicated
- lnf_bias: float32 [512], replicated
- w_head: bfloat16 [512, 50304], P(None, 'tp')
- b_head: float32 [50304], P('tp')
Outputs:
- output 1: float32 [], replicated
- output 2: bfloat16 [64, 1024, 512], P('dp')
- output 3: float32 [512], replicated
- output 4: float32 [512], replicated
- output 5: float32 [512, 8, 64], P(None, 'tp')
- output 6: float32 [512, 8, 64], P(None, 'tp')
- output 7: float32 [512, 8, 64], P(None, 'tp')
- output 8: float32 [8, 64, 512], P('tp')
- output 9: float32 [512, 2048], P(None, 'tp')
- output 10: float32 [2048], P('tp')
- output 11: float32 [2048, 512], P('tp')
- output 12: float32 [512], replicated
- output 13: float32 [512], replicated
- output 14: float32 [512], replicated
- output 15: float32 [512, 50304], P(None, 'tp')
- output 16: float32 [50304], P('tp')
All inputs are finite; a program needn't handle non-finite values.
Results may differ from the reference program's by a relative error of at most 0.0132186.
Values sent between devices are 32-bit elements.
A program may use at most 1 GiB of HBM per device.

```python
import jax
import jax.numpy as jnp
from jax import lax

BATCH_ROWS = 64
SEQ_LEN = 1024
D_MODEL = 512
N_HEADS = 8
HEAD_DIM = 64
FF_DIM = 2048
VOCAB_SIZE = 50304
ROT_DIM = HEAD_DIM // 4
LN_EPS = 1e-5
ROPE_BASE = 10000.0


def setup_inputs(seed: int = 0) -> dict:
    keys = jax.random.split(jax.random.key(seed), 17)

    def normal(index, shape, scale):
        return jax.random.normal(keys[index], shape, jnp.float32) * scale

    row_ids = jnp.arange(BATCH_ROWS)
    lengths = jax.random.randint(keys[1], (BATCH_ROWS,), SEQ_LEN // 8, SEQ_LEN + 1)
    lengths = jnp.where(row_ids == 0, SEQ_LEN, lengths)
    lengths = jnp.where(row_ids == BATCH_ROWS - 1, SEQ_LEN // 8, lengths)
    loss_mask = (jnp.arange(SEQ_LEN)[None, :] < lengths[:, None]).astype(jnp.int32)
    labels = jax.random.randint(keys[2], (BATCH_ROWS, SEQ_LEN), 0, VOCAB_SIZE)
    labels = labels.at[0, 0].set(0).at[0, 1].set(VOCAB_SIZE - 1)
    d_scale = D_MODEL ** -0.5
    return {
        'hidden': normal(0, (BATCH_ROWS, SEQ_LEN, D_MODEL), 1.0).astype(jnp.bfloat16),
        'labels': labels,
        'loss_mask': loss_mask,
        'ln_gain': 1.0 + normal(3, (D_MODEL,), 0.3),
        'ln_bias': normal(4, (D_MODEL,), 0.3),
        'w_query': normal(5, (D_MODEL, N_HEADS, HEAD_DIM), d_scale).astype(jnp.bfloat16),
        'w_key': normal(6, (D_MODEL, N_HEADS, HEAD_DIM), d_scale).astype(jnp.bfloat16),
        'w_value': normal(7, (D_MODEL, N_HEADS, HEAD_DIM), d_scale).astype(jnp.bfloat16),
        'w_attn_out': normal(8, (N_HEADS, HEAD_DIM, D_MODEL), d_scale).astype(jnp.bfloat16),
        'w_fc_in': normal(9, (D_MODEL, FF_DIM), d_scale).astype(jnp.bfloat16),
        'b_fc_in': normal(10, (FF_DIM,), 0.5),
        'w_fc_out': normal(11, (FF_DIM, D_MODEL), FF_DIM ** -0.5).astype(jnp.bfloat16),
        'b_fc_out': normal(12, (D_MODEL,), 0.5),
        'lnf_gain': 1.0 + normal(13, (D_MODEL,), 0.3),
        'lnf_bias': normal(14, (D_MODEL,), 0.3),
        'w_head': normal(15, (D_MODEL, VOCAB_SIZE), d_scale).astype(jnp.bfloat16),
        'b_head': normal(16, (VOCAB_SIZE,), 1.0) + jnp.linspace(-3.0, 3.0, VOCAB_SIZE),
    }


def bf16_grid(values):
    return values.astype(jnp.bfloat16).astype(jnp.float32)


def layer_norm(values, gain_vec, shift_vec):
    row_mean = jnp.mean(values, axis=-1, keepdims=True)
    centered = values - row_mean
    variance = jnp.mean(centered * centered, axis=-1, keepdims=True)
    return centered * lax.rsqrt(variance + LN_EPS) * gain_vec + shift_vec


def rope_tables(seq_count, rot_dim):
    half_rot = rot_dim // 2
    inv_freq = ROPE_BASE ** (-2.0 * jnp.arange(half_rot, dtype=jnp.float32) / rot_dim)
    angles = jnp.arange(seq_count, dtype=jnp.float32)[:, None] * inv_freq[None, :]
    return jnp.cos(angles)[:, None, :], jnp.sin(angles)[:, None, :]


def apply_rotary(tensor, cosine, sine_tab):
    rot_dim = 2 * cosine.shape[-1]
    pairs = tensor[..., :rot_dim].reshape(tensor.shape[:-1] + (rot_dim // 2, 2))
    even_part = pairs[..., 0]
    odd_part = pairs[..., 1]
    rotated = jnp.stack([even_part * cosine - odd_part * sine_tab, odd_part * cosine + even_part * sine_tab], axis=-1)
    return jnp.concatenate([rotated.reshape(tensor.shape[:-1] + (rot_dim,)), tensor[..., rot_dim:]], axis=-1)


def row_loss(params, hidden_row, label_row, mask_row, inv_count):
    (ln_gain, ln_bias, w_query, w_key, w_value, w_attn_out, w_fc_in, b_fc_in,
     w_fc_out, b_fc_out, lnf_gain, lnf_bias, w_head, b_head) = params
    seq_count = hidden_row.shape[0]
    cosine, sine_tab = rope_tables(seq_count, ROT_DIM)
    normed = bf16_grid(layer_norm(hidden_row, ln_gain, ln_bias))
    q_rot = bf16_grid(apply_rotary(jnp.einsum('td,dhe->the', normed, w_query), cosine, sine_tab))
    k_rot = bf16_grid(apply_rotary(jnp.einsum('td,dhe->the', normed, w_key), cosine, sine_tab))
    v_proj = bf16_grid(jnp.einsum('td,dhe->the', normed, w_value))
    causal = jnp.arange(seq_count)[None, :] <= jnp.arange(seq_count)[:, None]
    scores = jnp.einsum('qhe,khe->hqk', q_rot, k_rot) * (HEAD_DIM ** -0.5)
    probs = bf16_grid(jax.nn.softmax(jnp.where(causal[None], scores, -1e30), axis=-1))
    context = bf16_grid(jnp.einsum('hqk,khe->qhe', probs, v_proj))
    attn_out = jnp.einsum('qhe,hed->qd', context, w_attn_out)
    gelu_out = bf16_grid(jax.nn.gelu(jnp.dot(normed, w_fc_in) + b_fc_in, approximate=True))
    resid_out = hidden_row + attn_out + jnp.dot(gelu_out, w_fc_out) + b_fc_out
    final_norm = bf16_grid(layer_norm(resid_out, lnf_gain, lnf_bias))
    logits = jnp.dot(final_norm, w_head) + b_head
    log_norm = jax.nn.logsumexp(logits, axis=-1)
    target_logit = jnp.take_along_axis(logits, label_row[:, None], axis=-1)[:, 0]
    return jnp.sum(mask_row.astype(jnp.float32) * (log_norm - target_logit)) * inv_count


def reference(hidden, labels, loss_mask, ln_gain, ln_bias, w_query, w_key, w_value, w_attn_out,
              w_fc_in, b_fc_in, w_fc_out, b_fc_out, lnf_gain, lnf_bias, w_head, b_head):
    params = tuple(leaf.astype(jnp.float32) for leaf in (
        ln_gain, ln_bias, w_query, w_key, w_value, w_attn_out, w_fc_in, b_fc_in,
        w_fc_out, b_fc_out, lnf_gain, lnf_bias, w_head, b_head))
    inv_count = 1.0 / jnp.sum(loss_mask.astype(jnp.float32))
    checked = jax.checkpoint(row_loss)

    def total_loss(param_tuple, hidden_f32):
        per_row = lax.map(
            lambda row_args: checked(param_tuple, row_args[0], row_args[1], row_args[2], inv_count),
            (hidden_f32, labels, loss_mask))
        return jnp.sum(per_row)

    loss, vjp_fn = jax.vjp(total_loss, params, hidden.astype(jnp.float32))
    grads, grad_hidden = vjp_fn(jnp.ones_like(loss))
    (g_ln_gain, g_ln_bias, g_w_query, g_w_key, g_w_value, g_w_attn_out, g_w_fc_in, g_b_fc_in,
     g_w_fc_out, g_b_fc_out, g_lnf_gain, g_lnf_bias, g_w_head, g_b_head) = grads
    return (loss, grad_hidden.astype(jnp.bfloat16), g_ln_gain, g_ln_bias, g_w_query, g_w_key, g_w_value,
            g_w_attn_out, g_w_fc_in, g_b_fc_in, g_w_fc_out, g_b_fc_out, g_lnf_gain, g_lnf_bias,
            g_w_head, g_b_head)
```

```python
import functools
import jax
import jax.numpy as jnp
import numpy as np
from jax import lax
from jax.experimental import pallas as pl
from jax.experimental.pallas import tpu as pltpu
from jax.sharding import Mesh, PartitionSpec as P

F32, BF16 = jnp.float32, jnp.bfloat16
NT = (((1,), (1,)), ((), ()))
NN = (((1,), (0,)), ((), ()))
TN = (((0,), (0,)), ((), ()))
NEG = -1e30
LN_EPS = 1e-5
ROPE_BASE = 10000.0
LANES, SUBLANES = 128, 8
MICROSECOND = 1_000_000_000
ZERO, ONE, TWO, RING = 0, 1, 2, 4
DP = ('z', 'y', 'x')
DATA_SPECS = (P(DP, None, None), P(DP, None), P(DP, None))
PARAM_SPECS = (P(None), P(None), P(None, 'tp', None), P(None, 'tp', None), P(None, 'tp', None),
               P('tp', None, None), P(None, 'tp'), P('tp'), P('tp', None), P(None), P(None), P(None),
               P(None, 'tp'), P('tp'))
TURNS = (1, 3)
RIGHT, LEFT, _ = ([(i, (i + turn) % RING) for i in range(RING)] for turn in (*TURNS, TWO))
SWAP = [(0, 1), (1, 0)]
UNIT = 200
PIECE = RING * UNIT
HALF_SLICE = RING * PIECE
SLICE = TWO * HALF_SLICE
ORDERS = (('x', 'y', 'z'), ('y', 'z', 'x'), ('z', 'x', 'y'))
PARTS = ((72, 0, 0, 0, 0), (64, 72, 0, 0, 1), (64, 136, 0, 1, 0), (64, 0, 1, 1, 1), (64, 64, 1, 2, 0), (72, 128, 1, 2, 1))
BLOCK = ((16, 0), (8, 0), (16, 1), (16, 2))
HALVES = (pl.ds(0, 2), pl.ds(2, 2))
MESH_ID = pl.DeviceIdType.MESH
ANY, WHOLE, SCALARS = (pl.BlockSpec(memory_space=space) for space in (pl.ANY, pltpu.VMEM, pltpu.SMEM))


def dot(a, b, dims):
    return lax.dot_general(a, b, dims, preferred_element_type=F32)


def iota(shape, axis, dtype=jnp.int32):
    return lax.broadcasted_iota(dtype, shape, axis)


def params(collective=None):
    return pltpu.CompilerParams(vmem_limit_bytes=60 * 2 ** 20, collective_id=collective, has_side_effects=collective is not None)


def cost(us, transfer=1):
    return pl.CostEstimate(flops=us * MICROSECOND, bytes_accessed=transfer, transcendentals=1)


def struct(shape, dtype=F32):
    return jax.ShapeDtypeStruct(shape, dtype)


def origin(*_):
    return (0, 0)


def row_block(i, *_):
    return (i, 0)


def column_block(i, *_):
    return (0, i)


def chunks(total, size=LANES):
    return [slice(at, at + size) for at in range(ZERO, total, size)]


def as_row(column):
    return jnp.transpose(jnp.broadcast_to(column, (column.shape[0], LANES)))[0:1]


def head_lse(z, w_t, bias, begin=None, tile=2560, sub=512):
    tokens, dim = z.shape
    vocab = w_t.shape[0]
    steps = pl.cdiv(vocab, tile)
    early = steps // TWO
    offset = ZERO if begin is None else early

    def kernel(z_ref, w_ref, b_ref, *refs):
        step = pl.program_id(ZERO) + offset
        *begins, m_ref, s_ref = refs
        out_ref = begins.pop() if begins else None

        @pl.when(step == offset)
        def _():
            m_ref[...] = begins[0][...] if begins else jnp.full_like(m_ref, NEG)
            s_ref[...] = begins[1][...] if begins else jnp.zeros_like(s_ref)

        def work(last):
            zz = z_ref[...]
            for part in chunks(tile, sub):
                l = dot(zz, w_ref[part, :], NT) + b_ref[:, part]
                if last:
                    l = jnp.where(iota(l.shape, ONE) < vocab - step * tile - part.start, l, NEG)
                lanes = [l[:, c] for c in chunks(sub)]
                m_old = m_ref[...]
                m_new = jnp.maximum(m_old, functools.reduce(jnp.maximum, lanes))
                s_ref[...] = s_ref[...] * jnp.exp(m_old - m_new) + sum(jnp.exp(x - m_new) for x in lanes)
                m_ref[...] = m_new

        pl.when(step < steps - ONE)(lambda: work(last=False))

        @pl.when(step == steps - ONE)
        def _():
            if out_ref is None:
                return
            work(last=True)
            top = jnp.max(m_ref[...], axis=ONE, keepdims=True)
            total = jnp.sum(s_ref[...] * jnp.exp(m_ref[...] - top), axis=ONE, keepdims=True)
            out_ref[0:1] = as_row(top)
            out_ref[1:2] = as_row(total)

    state = pl.BlockSpec((tokens, LANES), origin)
    first = begin is None
    return pl.pallas_call(
        kernel, grid=(early if first else steps - early,),
        in_specs=[pl.BlockSpec((tokens, dim), origin), pl.BlockSpec((tile, dim), lambda i: (i + offset, ZERO)),
                  pl.BlockSpec((ONE, tile), lambda i: (ZERO, i + offset))] + ([] if first else [state] * TWO),
        out_specs=[state] * TWO if first else pl.BlockSpec((TWO, tokens), origin),
        out_shape=[struct((tokens, LANES))] * TWO if first else struct((TWO, tokens)),
        scratch_shapes=[] if first else [pltpu.VMEM((tokens, LANES), F32)] * TWO,
        compiler_params=params(), cost_estimate=cost(19), name='head_lse_first' if first else 'head_lse_rest',
    )(z, w_t, bias, *(begin or ()))


def head_gz(z, w_t, bias, lse, tag, tile=2560, sub=2560):
    tokens, dim = z.shape
    vocab = w_t.shape[0]
    steps = pl.cdiv(vocab, tile)

    def kernel(z_ref, w_ref, b_ref, lse_ref, tag_ref, gz_ref, t_ref, gb_ref):
        step = pl.program_id(ZERO)

        @pl.when(step == ZERO)
        def _():
            gz_ref[...] = jnp.zeros_like(gz_ref)
            t_ref[...] = jnp.zeros_like(t_ref)

        def work(last):
            zz = z_ref[...]
            lane = iota((tokens, LANES), ONE)
            for part in chunks(tile, sub):
                w = w_ref[part, :]
                left = vocab - step * tile - part.start
                if last:
                    w = jnp.where(iota(w.shape, ZERO) < left, w, jnp.zeros_like(w))
                l = dot(zz, w, NT) + b_ref[:, part]
                norm, rel = lse_ref[...], tag_ref[...] - (step * tile + part.start)
                grads, targets = [], []
                for c in chunks(sub):
                    hit = lane == rel - c.start
                    prob = jnp.exp(l[:, c] - norm)
                    if last:
                        prob = jnp.where(lane < left - c.start, prob, 0.0)
                    grads.append(prob - jnp.where(hit, 1.0, 0.0))
                    targets.append(jnp.where(hit, l[:, c], 0.0))
                t_ref[...] += sum(targets)
                grad = jnp.concatenate(grads, axis=ONE)
                gb_ref[:, part] = jnp.sum(grad.reshape(-1, SUBLANES, sub), axis=ZERO)
                gz_ref[...] += dot(grad.astype(BF16), w, NN)

        pl.when(step < steps - ONE)(lambda: work(last=False))
        pl.when(step == steps - ONE)(lambda: work(last=True))

    narrow = pl.BlockSpec((tokens, LANES), origin)
    return pl.pallas_call(
        kernel, grid=(steps,),
        in_specs=[pl.BlockSpec((tokens, dim), origin), pl.BlockSpec((tile, dim), row_block), pl.BlockSpec((ONE, tile), column_block),
                  narrow, narrow],
        out_specs=[pl.BlockSpec((tokens, dim), origin), narrow, pl.BlockSpec((SUBLANES, tile), column_block)],
        out_shape=[struct((tokens, dim)), struct((tokens, LANES)), struct((SUBLANES, steps * tile))],
        compiler_params=params(), cost_estimate=cost(72), name='head_gz',
    )(z, w_t, bias, lse, tag)


def swap_pairs(x, even):
    return jnp.where(even, pltpu.roll(x, LANES - ONE, ONE), pltpu.roll(x, ONE, ONE))


def halves_of(value, low):
    empty = jnp.zeros_like(value)
    return jnp.where(low, value, empty), jnp.where(low, empty, value)


def attn_fwd(u, wq, wk, wv, cos_t, sin_t, scale, blk=256):
    tokens, dim = u.shape
    lanes = wq.shape[0]

    def kernel(u_ref, wq_ref, wk_ref, wv_ref, c_ref, s_ref, qs_ref, k_ref, v_ref, ctx_ref, lse_ref):
        uu, cc, ss = u_ref[...], c_ref[...], s_ref[...]
        even = iota((tokens, LANES), ONE) % TWO == ZERO
        q = dot(uu, wq_ref[...], NT)
        qs_ref[...] = ((q * cc + swap_pairs(q, even) * ss).astype(BF16).astype(F32) * scale).astype(BF16)
        k = dot(uu, wk_ref[...], NT)
        k_ref[...] = (k * cc + swap_pairs(k, even) * ss).astype(BF16)
        v_ref[...] = dot(uu, wv_ref[...], NT).astype(BF16)
        low = iota((blk, LANES), ONE) < LANES // TWO
        causal = iota((blk, blk), ONE) <= iota((blk, blk), ZERO)
        for rows in chunks(tokens, blk):
            before, keys = slice(rows.start), slice(rows.stop)
            out = []
            for h, qh in enumerate(halves_of(qs_ref[rows, :], low)):
                s = jnp.where(causal, dot(qh, k_ref[rows, :], NT), NEG)
                if rows.start:
                    s = jnp.concatenate([dot(qh, k_ref[before, :], NT), s], axis=ONE)
                m = jnp.max(s, axis=ONE, keepdims=True)
                e = jnp.exp(s - m)
                l = jnp.sum(e, axis=ONE, keepdims=True)
                out.append(dot((e * (1.0 / l)).astype(BF16), v_ref[keys, :], NN))
                lse_ref[ZERO, h:h + ONE, rows] = as_row(m + jnp.log(l))
            ctx_ref[rows, :] = jnp.where(low, *out).astype(BF16)

    pair, wide = pl.BlockSpec((tokens, LANES), column_block), pl.BlockSpec((tokens, LANES), origin)
    return pl.pallas_call(
        kernel, grid=(lanes // LANES,),
        in_specs=[pl.BlockSpec((tokens, dim), origin)] + [pl.BlockSpec((LANES, dim), row_block)] * 3 + [wide] * TWO,
        out_specs=[pair] * RING + [pl.BlockSpec((ONE, TWO, tokens), lambda g: (g, ZERO, ZERO))],
        out_shape=[struct((tokens, lanes), BF16)] * RING + [struct((lanes // LANES, TWO, tokens))],
        compiler_params=params(), cost_estimate=cost(13), name='attn_fwd',
    )(u, wq, wk, wv, cos_t, sin_t)


def attn_bwd(qs, k, v, dctx, lse, cos_t, sin_t, scale, blk=256):
    tokens, lanes = qs.shape

    def kernel(qs_ref, k_ref, v_ref, do_ref, lse_ref, c_ref, s_ref, dq_ref, dk_ref, dv_ref, dka_ref, dva_ref):
        low = iota((blk, LANES), ONE) < LANES // TWO
        causal = iota((blk, blk), ZERO) <= iota((blk, blk), ONE)
        even = iota((blk, LANES), ONE) % TWO == ZERO

        def unrotate(x, rows):
            return (x * c_ref[rows, :] - swap_pairs(x, even) * s_ref[rows, :]).astype(BF16)

        dka_ref[...] = jnp.zeros_like(dka_ref)
        dva_ref[...] = jnp.zeros_like(dva_ref)
        for rows in chunks(tokens, blk):
            before, keys = slice(rows.start), slice(rows.stop)
            dqs = []
            for h, (qh, doh) in enumerate(zip(halves_of(qs_ref[rows, :], low), halves_of(do_ref[rows, :], low))):
                norm = lse_ref[ZERO, h:h + ONE, rows]
                p = jnp.where(causal, jnp.exp(dot(k_ref[rows, :], qh, NT) - norm), 0.0)
                if rows.start:
                    p = jnp.concatenate([jnp.exp(dot(k_ref[before, :], qh, NT) - norm), p], axis=ZERO)
                dp = dot(v_ref[keys, :], doh, NT)
                ds = (p * (dp - jnp.sum(p * dp, axis=ZERO, keepdims=True))).astype(BF16)
                dva_ref[keys, :] += dot(p.astype(BF16), doh, NN)
                dka_ref[keys, :] += dot(ds, qh, NN)
                dqs.append(dot(ds, k_ref[keys, :], TN))
            dq_ref[rows, :] = unrotate(jnp.where(low, *dqs) * scale, rows)
        for rows in chunks(tokens, blk):
            dk_ref[rows, :] = unrotate(dka_ref[rows, :], rows)
            dv_ref[rows, :] = dva_ref[rows, :].astype(BF16)

    pair, wide = pl.BlockSpec((tokens, LANES), column_block), pl.BlockSpec((tokens, LANES), origin)
    return pl.pallas_call(
        kernel, grid=(lanes // LANES,),
        in_specs=[pair] * RING + [pl.BlockSpec((ONE, TWO, tokens), lambda g: (g, ZERO, ZERO))] + [wide] * TWO,
        out_specs=[pair] * 3, out_shape=[struct((tokens, lanes), BF16)] * 3,
        scratch_shapes=[pltpu.VMEM((tokens, LANES), F32)] * TWO,
        compiler_params=params(), cost_estimate=cost(13), name='attn_bwd',
    )(qs, k, v, dctx, lse, cos_t, sin_t)


class Wires:
    def __init__(self, send, recv):
        self.send, self.recv, self.all = send, recv, []

    def line(self, src, dst, axis, turn):
        n = len(self.all)

        def build():
            size = TWO if axis == 'tp' else RING
            peer = {axis: lax.rem(lax.axis_index(axis) + turn, size)}
            return pltpu.make_async_remote_copy(src(), dst(), self.send.at[n], self.recv.at[n], device_id=peer, device_id_type=MESH_ID)

        self.all.append(build)
        return build

    def finish(self):
        for build in self.all:
            build().wait_send()


def start(lines):
    for build in lines:
        build().start()


def arrive(lines):
    for build in lines:
        build().wait_recv()


def greet(peers):
    barrier = pltpu.get_barrier_semaphore()
    for peer in peers:
        where = {axis: lax.rem(lax.axis_index(axis) + turn, TWO if axis == 'tp' else RING) for axis, turn in peer}
        pl.semaphore_signal(barrier, device_id=where, device_id_type=MESH_ID)
    return lambda: pl.semaphore_wait(barrier, len(peers))


class RingSum:
    def __init__(self, wires, axis, piece, halves, near, far):
        self.piece, self.halves, self.near, self.far = piece, halves, near, far
        sent = lambda part, s, turn: piece(turn).at[part[s]]
        kept = lambda part, s: far[s].at[part[s]]
        self.first = [wires.line(functools.partial(sent, halves, s, TWO), functools.partial(lambda s: near[s], s), axis, turn)
                      for s, turn in enumerate(TURNS)]
        self.plain, self.added = ([wires.line(functools.partial(sent, part, s, turn), functools.partial(kept, part, s), axis, turn)
                                   for s, turn in enumerate(TURNS)] for part in (halves[::-1], halves))

    def relay(self):
        for s, turn in enumerate(TURNS):
            arrive([self.first[s]])
            part = self.piece(turn).at[self.halves[s]]
            part[...] = part[...] + self.near[s][...]
            start([self.added[s]])

    def result(self):
        arrive(self.plain + self.added)
        return self.piece(ZERO)[...] + (self.far[0][...] + self.far[1][...])


class FanSum:
    def __init__(self, wires, axis, piece, landing):
        self.piece, self.landing = piece, landing
        self.lines = [wires.line(functools.partial(piece, turn), functools.partial(lambda n: landing.at[n], turn - ONE), axis, turn)
                      for turn in range(ONE, RING)]

    def result(self):
        arrive(self.lines)
        return self.piece(ZERO)[...] + (self.landing[0] + self.landing[1] + self.landing[2])


class RingGather:
    def __init__(self, wires, axis, place, relays):
        here = functools.partial(place, ZERO)
        self.step = [wires.line(here, here, axis, turn) for turn in TURNS]
        self.came, self.relays = [], []
        for way, part in relays:
            passed = functools.partial(lambda way, part: place(TURNS[ONE - way]).at[part], way, part)
            self.relays.append((way, wires.line(passed, passed, axis, TURNS[way])))
        self.idle = [s for s in range(TWO) if s not in dict(relays)]

    def forward(self):
        for way, line in self.relays:
            arrive([self.step[way]])
            start([line])

    def result(self):
        arrive([self.step[s] for s in self.idle] + [line for _, line in self.relays])


class FanGather:
    def __init__(self, wires, axis, place):
        here = functools.partial(place, ZERO)
        self.step = [wires.line(here, here, axis, turn) for turn in range(ONE, RING)]

    def result(self):
        arrive(self.step)


def coordinates():
    at = {axis: lax.axis_index(axis) for axis in DP}
    return at, lambda axis, turn: lax.rem(at[axis] + turn, RING)


def head_gw(stats, packets, w_t, bias_cols):
    tokens = stats.shape[1]
    dim = w_t.shape[1]
    vocab = w_t.shape[0]
    half = tokens // TWO
    low = 104
    halves = (pl.ds(ZERO, low), pl.ds(low, UNIT - low))
    colors = (('y', 'z'), ('z', 'y'))
    group = [(x, c) for c in range(TWO) for x in range(RING)][1:]
    firsts = [ZERO] * RING + [packets[3].shape[0]]

    def spot(ref, n):
        return ref.at[min(n, 3), pl.ds(firsts[n], packets[n].shape[0])]

    def kernel(stats_ref, *refs):
        packet_refs, (w_ref, bias_ref), refs = refs[:len(packets)], refs[len(packets):len(packets) + TWO], refs[len(packets) + TWO:]
        outs, (count_out, norm_out), refs = refs[:len(PARTS)], refs[len(PARTS):len(PARTS) + TWO], refs[len(PARTS) + TWO:]
        (acc, w_all, zb, own, theirs, heard, norms, tags, shard, tally, *lanes, send, recv, local) = refs
        at, beside = coordinates()
        tp = lax.axis_index('tp')
        wires = Wires(send, recv)

        entered = greet([(('x', x), ('tp', c)) for x, c in group] + [((a, t),) for a in ('y', 'z') for t in range(ONE, RING)])
        loads = [pltpu.make_async_copy(ref, spot(own, n), local.at[n]) for n, ref in enumerate(packet_refs)]
        for load in loads:
            load.start()
        for n in range(TWO * RING):
            row = pl.multiple_of(at['x'] * SLICE + n * PIECE, 32)
            whole = row + PIECE <= vocab

            @pl.when(whole)
            def _():
                pltpu.make_async_copy(w_ref.at[pl.ds(row, PIECE)], w_all.at[n], local.at[len(packets) + n]).start()

            @pl.when(jnp.logical_not(whole))
            def _():
                pltpu.make_async_copy(w_ref.at[pl.ds(row, vocab % PIECE)], w_all.at[n, pl.ds(ZERO, vocab % PIECE)], local.at[len(packets) + n]).start()
        entered()
        news = []
        for n, (x, c) in enumerate(group):
            where = {'x': beside('x', x), 'tp': lax.rem(tp + c, TWO)}
            news.append(pltpu.make_async_remote_copy(stats_ref, heard.at[n + ONE], send.at[n], recv.at[n], device_id=where, device_id_type=MESH_ID))
            wires.all.append(functools.partial(lambda n: news[n], n))
            news[n].start()
        swaps = [wires.line(functools.partial(lambda n: packet_refs[n], n), functools.partial(spot, theirs, n), 'tp', ONE)
                 for n in range(len(packets))]
        start(swaps)
        mine = pl.multiple_of(tp * half, half)
        other = pl.multiple_of(half - tp * half, half)
        for load in loads:
            load.wait()
        for r in range(RING):
            zb[r, pl.ds(mine, half), :] = own[r, ZERO:half].astype(BF16)
        for copy in news:
            copy.wait_recv()
        heard[0] = stats_ref[...]
        for r, turn in enumerate((0, 1, 3, 2)):
            a, b = heard[turn], heard[turn + RING]
            top = jnp.maximum(a[0:1], b[0:1])
            norm = top + jnp.log(a[1:2] * jnp.exp(a[0:1] - top) + b[1:2] * jnp.exp(b[0:1] - top))
            label, mask = (jnp.concatenate([own[r, half + n:half + n + ONE] for n in (row, row + ONE)], axis=ONE) for row in (ZERO, TWO))
            norms[r] = jnp.where(mask > 0.0, norm, -NEG)
            tags[r] = jnp.where(mask > 0.0, label - (tp * vocab).astype(F32), NEG)
            seen = jnp.broadcast_to(jnp.sum(mask, axis=ONE, keepdims=True), tally.shape[1:])
            tally[6] = seen if r == ZERO else tally[6] + seen
            if r == ZERO:
                norm_out[...] = norm
        arrive(swaps)
        for r in range(RING):
            zb[r, pl.ds(other, half), :] = theirs[r, ZERO:half].astype(BF16)

        pieces = [functools.partial(lambda c, axis, turn: acc.at[c * RING + beside(axis, turn)], c, axis) for c, (axis, _) in enumerate(colors)]
        sums = [RingSum(wires, colors[c][0], pieces[c], HALVES, [lanes[0].at[c], lanes[1].at[c]], [lanes[2].at[c], lanes[3].at[c]])
                for c in range(TWO)]
        votes = FanSum(wires, 'y', lambda turn: tally.at[6], tally.at[pl.ds(0, 3)])

        def unit(u, carry):
            c, turn = lax.rem(u, TWO), lax.div(u, TWO)
            ahead = lax.rem(2 + 3 * turn + 3 * lax.div(turn * (turn - ONE), TWO), RING)
            p = c * RING + lax.rem(at['y'] + (at['z'] - at['y']) * c + ahead, RING)
            first_row = at['x'] * SLICE + p * PIECE
            whole = first_row + PIECE <= vocab

            @pl.when(whole)
            def _():
                pltpu.make_async_copy(w_ref.at[pl.ds(ZERO, PIECE)], w_all.at[p], local.at[len(packets) + p]).wait()

            @pl.when(jnp.logical_not(whole))
            def _():
                pltpu.make_async_copy(w_ref.at[pl.ds(ZERO, vocab % PIECE)], w_all.at[p, pl.ds(ZERO, vocab % PIECE)], local.at[len(packets) + p]).wait()

            w, bias = w_all[p], bias_ref[p]
            row = (iota((PIECE, LANES), ZERO) + first_row).astype(F32)

            logits = dot(w, zb[0], NT)
            for r in range(RING):
                zr, norm, tag, l = zb[r], norms[r], tags[r], logits
                if r + ONE < RING:
                    logits = dot(w, zb[r + ONE], NT)
                grads = []
                for part in chunks(tokens):
                    prob = jnp.exp(l[:, part] + bias - norm[:, part])
                    grads.append((prob - jnp.where(row == tag[:, part], 1.0, 0.0)).astype(BF16))
                out = dot(jnp.concatenate(grads, axis=ONE), zr, NN).reshape(RING, UNIT, dim)
                acc[p] = acc[p] + out if r else out
            for c, total in enumerate(sums):
                pl.when(u == c)(functools.partial(start, total.first))
                pl.when(u == c + TWO)(functools.partial(start, total.plain[:1]))

                @pl.when(u == c + RING)
                def _(total=total):
                    start(total.plain[1:])
                    total.relay()

            return carry

        start(votes.lines)
        lax.fori_loop(ZERO, TWO * RING, unit, ZERO)
        tally[7] = votes.result()
        votes = FanSum(wires, 'z', lambda turn: tally.at[7], tally.at[pl.ds(3, 3)])
        start(votes.lines)

        seconds = []
        for c, (axis, side) in enumerate(colors):
            kept = c * RING + at[axis]
            acc[kept] = sums[c].result()
            seconds.append(RingSum(wires, side, functools.partial(lambda kept, side, turn: acc.at[kept, beside(side, turn)], kept, side),
                                   halves, [lanes[4].at[c], lanes[5].at[c]], [lanes[6].at[c], lanes[7].at[c]]))
            start(seconds[c].first + seconds[c].plain)
        for total in seconds:
            total.relay()
        for c, total in enumerate(seconds):
            shard[c] = total.result()
        count_out[...] = votes.result()

        keep, steps = [], []
        for n, (rows, offset, c, order, way) in enumerate(PARTS):
            a1, a2, _ = ORDERS[order]
            source = shard.at[c, pl.ds(offset, rows)]
            home = functools.partial(lambda n, a1, a2, turn: outs[n].at[at[a2], beside(a1, turn)], n, a1, a2)
            keep.append(pltpu.make_async_copy(source, home(ZERO), local.at[len(packets) + TWO * RING + n]))
            keep[n].start()
            gather = RingGather(wires, a1, home, [(way, pl.ds(ZERO, rows))])
            steps.append(gather)
        for copy in keep:
            copy.wait()
        for gather in steps:
            start(gather.step)
        for gather in steps:
            gather.forward()
        nexts = []
        for n, (rows, _, _, order, way) in enumerate(PARTS):
            _, a2, _ = ORDERS[order]
            steps[n].result()
            nexts.append(RingGather(wires, a2, functools.partial(lambda n, a2, turn: outs[n].at[beside(a2, turn)], n, a2), [(way, pl.ds(ZERO, RING))]))
            start(nexts[n].step)
        for gather in nexts:
            gather.forward()
        for gather in nexts:
            gather.result()
        wires.finish()

    copies = len(group) + len(packets) + TWO * 3 + TWO * TWO * 6 + len(PARTS) * TWO * 3
    row_vector = pltpu.VMEM((RING, ONE, tokens), F32)
    packet = pltpu.VMEM((RING, *packets[0].shape), F32)
    lane = lambda *shape: [pltpu.VMEM((TWO, *shape, dim), F32)]
    return pl.pallas_call(
        kernel, in_specs=[WHOLE] + [ANY] * len(packets) + [ANY, WHOLE], out_specs=[ANY] * len(PARTS) + [WHOLE] * TWO,
        out_shape=[struct((RING, RING, part[0], dim)) for part in PARTS] + [struct((SUBLANES, LANES)), struct((ONE, tokens))],
        scratch_shapes=[pltpu.VMEM((TWO * RING, RING, UNIT, dim), F32), pltpu.VMEM((TWO * RING, PIECE, dim), BF16),
                        pltpu.VMEM((RING, tokens, dim), BF16), packet, packet, pltpu.VMEM((TWO * RING, TWO, tokens), F32),
                        row_vector, row_vector, pltpu.VMEM((TWO, UNIT, dim), F32), pltpu.VMEM((TWO * RING, SUBLANES, LANES), F32),
                        *lane(TWO, UNIT) * TWO, *lane(RING, UNIT) * TWO, *lane(low), *lane(UNIT - low), *lane(UNIT) * TWO,
                        pltpu.SemaphoreType.DMA((copies,)), pltpu.SemaphoreType.DMA((copies,)),
                        pltpu.SemaphoreType.DMA((len(packets) + TWO * RING + len(PARTS),))],
        compiler_params=params(1), cost_estimate=cost(160), name='head_gw',
    )(stats, *packets, w_t, bias_cols)


def chip_sum(inputs):
    count = len(BLOCK)
    flat = [piece for group in inputs for piece in group]
    dim = flat[0].shape[-1]

    def kernel(*refs):
        ins, outs, refs = refs[:len(flat)], refs[len(flat):len(flat) + count], refs[len(flat) + count:]
        acc, bufs, (send, recv, local) = refs[:count], [refs[count * n:count * (n + ONE)] for n in range(ONE, 7)], refs[-3:]
        at, beside = coordinates()
        wires = Wires(send, recv)
        entered = greet([((a, t),) for a in DP for t in range(ONE, RING)])
        loads, used = [[] for _ in BLOCK], ZERO
        for k, group in enumerate(inputs):
            row = ZERO
            for piece in group:
                rows = piece.shape[0]
                loads[k].append(pltpu.make_async_copy(ins[used], acc[k].at[pl.ds(row, rows)], local.at[used]))
                loads[k][-1].start()
                row, used = row + rows, used + ONE
        entered()
        stages = []
        for k, (_, order) in enumerate(BLOCK):
            a1 = ORDERS[order][0]
            stages.append(RingSum(wires, a1, functools.partial(lambda k, a1, turn: acc[k].at[beside(a1, turn)], k, a1),
                                  HALVES, [bufs[0][k], bufs[1][k]], [bufs[2][k], bufs[3][k]]))
            for load in loads[k]:
                load.wait()
            start(stages[k].first + stages[k].plain)
        for stage in stages:
            stage.relay()
        for k, (_, order) in enumerate(BLOCK):
            a1, a2, _ = ORDERS[order]
            acc[k][at[a1]] = stages[k].result()
            stages[k] = FanSum(wires, a2, functools.partial(lambda k, a1, a2, turn: acc[k].at[at[a1], beside(a2, turn)], k, a1, a2), bufs[4][k])
            start(stages[k].lines)
        for k, (_, order) in enumerate(BLOCK):
            a1, a2, a3 = ORDERS[order]
            acc[k][at[a1], at[a2]] = stages[k].result()
            stages[k] = FanSum(wires, a3, functools.partial(lambda k, a1, a2, a3, turn: acc[k].at[at[a1], at[a2], beside(a3, turn)], k, a1, a2, a3), bufs[5][k])
            start(stages[k].lines)
        for k, (_, order) in enumerate(BLOCK):
            a1, a2, a3 = ORDERS[order]
            outs[k][at[a1], at[a2], at[a3]] = stages[k].result()
            stages[k] = FanGather(wires, a3, functools.partial(lambda k, a1, a2, a3, turn: outs[k].at[at[a1], at[a2], beside(a3, turn)], k, a1, a2, a3))
            start(stages[k].step)
        for k, (_, order) in enumerate(BLOCK):
            a1, a2, _ = ORDERS[order]
            stages[k].result()
            stages[k] = FanGather(wires, a2, functools.partial(lambda k, a1, a2, turn: outs[k].at[at[a1], beside(a2, turn)], k, a1, a2))
            start(stages[k].step)
        for k, (_, order) in enumerate(BLOCK):
            a1 = ORDERS[order][0]
            stages[k].result()
            stages[k] = RingGather(wires, a1, functools.partial(lambda k, a1, turn: outs[k].at[beside(a1, turn)], k, a1), list(enumerate(HALVES)))
            start(stages[k].step)
        for stage in stages:
            stage.forward()
        for stage in stages:
            stage.result()
        wires.finish()

    copies = count * (6 + 3 * RING + RING)

    def buffers(*shape):
        return [pltpu.VMEM((*shape, rows, dim), F32) for rows, _ in BLOCK]

    return pl.pallas_call(
        kernel, in_specs=[ANY] * len(flat), out_specs=[WHOLE] * count,
        out_shape=[struct((RING, RING, RING, rows, dim)) for rows, _ in BLOCK],
        scratch_shapes=[*buffers(RING, RING, RING), *buffers(TWO, RING) * TWO, *buffers(RING, RING) * TWO, *buffers(3, RING), *buffers(3),
                        pltpu.SemaphoreType.DMA((copies,)), pltpu.SemaphoreType.DMA((copies,)), pltpu.SemaphoreType.DMA((len(flat),))],
        compiler_params=params(2), cost_estimate=cost(60), name='chip_sum',
    )(*flat)


def place(groups, scale, coords, vocab, into=None):
    jobs = [(shift, n, array) for shift, arrays in groups for n, array in arrays.items()]
    dim = jobs[0][-1].shape[-1]
    steps = RING * RING
    kept = () if into is None else (into,)

    def kernel(coord_ref, scale_ref, *refs):
        ins, (out_ref, bufs, sems) = refs[:len(jobs)], refs[-3:]
        step = pl.program_id(ZERO)

        def each(step, act):
            slot = lax.rem(step, TWO)
            for j, (shift, n, _) in enumerate(jobs):
                rows, offset, c, order, _ = PARTS[n]
                a1, a2, a3 = ORDERS[order]
                at = {a1: lax.rem(step, RING), a2: lax.div(step, RING), a3: lax.rem(coord_ref[DP.index(a3)] + shift, RING)}
                first, second = (('y', 'z'), ('z', 'y'))[c]
                row = pl.multiple_of(at['x'] * SLICE + c * HALF_SLICE + at[first] * PIECE + at[second] * UNIT + offset, SUBLANES)
                edge = vocab % UNIT - offset
                whole = row + rows <= vocab

                def move(size):
                    act(pltpu.make_async_copy(bufs.at[slot, j, pl.ds(ZERO, size)], out_ref.at[pl.ds(row, size)], sems.at[slot, j]))

                pl.when(whole)(functools.partial(move, rows))
                if ZERO < edge < rows:
                    pl.when(jnp.logical_and(row < vocab, jnp.logical_not(whole)))(functools.partial(move, edge))

        @pl.when(step >= TWO)
        def _():
            each(step - TWO, lambda copy: copy.wait())

        for j, (_, n, _) in enumerate(jobs):
            bufs[lax.rem(step, TWO), j, ZERO:PARTS[n][0]] = ins[j][ZERO, ZERO] * scale_ref[ZERO]
        each(step, lambda copy: copy.start())

        @pl.when(step == steps - ONE)
        def _():
            each(step - ONE, lambda copy: copy.wait())
            each(step, lambda copy: copy.wait())

    blocks = [pl.BlockSpec((ONE, ONE, PARTS[n][0], dim), lambda i: (i // RING, i % RING, ZERO, ZERO)) for _, n, _ in jobs]
    return pl.pallas_call(
        kernel, grid=(steps,), in_specs=[SCALARS, SCALARS, *blocks] + [ANY for _ in kept], out_specs=ANY,
        out_shape=struct((vocab, dim)), input_output_aliases={TWO + len(jobs): ZERO for _ in kept},
        scratch_shapes=[pltpu.VMEM((TWO, len(jobs), 72, dim), F32), pltpu.SemaphoreType.DMA((TWO, len(jobs)))],
        compiler_params=params(), cost_estimate=cost(2 * len(jobs)),
    )(coords, scale, *[array for *_, array in jobs], *kept)


def norm_stats(values):
    row_mean = jnp.mean(values, axis=-ONE, keepdims=True)
    centered = values - row_mean
    inv_std = lax.rsqrt(jnp.mean(centered * centered, axis=-ONE, keepdims=True) + LN_EPS)
    return centered * inv_std, inv_std


def norm_backward(grad_out, x_hat, inv_std, gain_vec):
    grad_hat = grad_out * gain_vec
    mean_grad = jnp.mean(grad_hat, axis=-ONE, keepdims=True)
    mean_proj = jnp.mean(grad_hat * x_hat, axis=-ONE, keepdims=True)
    grad_in = inv_std * (grad_hat - mean_grad - x_hat * mean_proj)
    return grad_in, jnp.sum(grad_out * x_hat, axis=ZERO), jnp.sum(grad_out, axis=ZERO)


def rope_tables(tokens, head_dim):
    rot = head_dim // 4
    inv_freq = (ROPE_BASE ** (-2.0 * np.arange(rot // TWO) / rot)).astype(np.float32)
    angles = (np.arange(tokens, dtype=np.float32)[:, np.newaxis] * inv_freq).astype(np.float64)
    cosine, sine = np.ones((tokens, head_dim), np.float32), np.zeros((tokens, head_dim), np.float32)
    cosine[:, :rot] = np.repeat(np.cos(angles), TWO, axis=ONE)
    sine[:, :rot] = np.repeat(np.sin(angles), TWO, axis=ONE) * np.tile([-1.0, 1.0], rot // TWO)
    return [np.tile(table, (ONE, LANES // head_dim)) for table in (cosine, sine)]


def hop(value, axis, way):
    return lax.ppermute(value, axis, way)


def solution(mesh):
    mesh = Mesh(mesh.devices.reshape(TWO, RING, RING, RING), ('tp', *DP))

    def local_step(hidden, labels, loss_mask, ln_gain, ln_bias, w_query, w_key, w_value, w_attn_out,
                   w_fc_in, b_fc_in, w_fc_out, b_fc_out, lnf_gain, lnf_bias, w_head, b_head):
        _, tokens, dim = hidden.shape
        _, heads, head_dim = w_query.shape
        lanes, half = heads * head_dim, tokens // TWO
        vocab = b_head.shape[0]
        score_scale = head_dim ** -0.5
        tp = lax.axis_index('tp')
        swap = lambda value: lax.ppermute(value, 'tp', SWAP)
        rows_of = lambda w: jnp.moveaxis(w, ZERO, -ONE).reshape(lanes, dim)
        wq, wk, wv = rows_of(w_query), rows_of(w_key), rows_of(w_value)
        wo = w_attn_out.reshape(lanes, dim)
        w_t = w_head.T
        tables = rope_tables(tokens, head_dim)
        mask_f = loss_mask.astype(F32)

        resid_in = hidden[ZERO].astype(F32)
        ln_hat, ln_inv = norm_stats(resid_in)
        normed = (ln_hat * ln_gain + ln_bias).astype(BF16)
        qs, k_rot, v_proj, context, lse_att = attn_fwd(normed, wq, wk, wv, *tables, score_scale)
        pre_act = dot(normed, w_fc_in, NN) + b_fc_in
        gelu_out, gelu_vjp = jax.vjp(functools.partial(jax.nn.gelu, approximate=True), pre_act)
        gelu_bf = gelu_out.astype(BF16)
        block_part = dot(context, wo, NN) + dot(gelu_bf, w_fc_out, NN)
        resid_out = resid_in + (block_part + swap(block_part)) + b_fc_out
        fin_hat, fin_inv = norm_stats(resid_out)
        final_f32 = fin_hat * lnf_gain + lnf_bias
        final_bf = final_f32.astype(BF16)

        extra = jnp.concatenate([labels.astype(F32).reshape(TWO, half), mask_f.reshape(TWO, half), jnp.zeros((RING, half), F32)])
        packet = jnp.concatenate([lax.dynamic_slice_in_dim(final_f32, tp * half, half, ZERO), extra])
        from_sides = [hop(packet, 'x', way) for way in (RIGHT, LEFT)]
        cut = packet.shape[0] // TWO // SUBLANES * SUBLANES
        across = [hop(side, 'x', way)
                  for side, way in ((from_sides[0][:cut], RIGHT), (from_sides[1][cut:], LEFT))]

        bias_row = b_head[np.newaxis]
        bias_pad = jnp.concatenate([b_head, jnp.full((RING * SLICE - vocab,), NEG, F32)])
        bias_mine = lax.dynamic_slice_in_dim(bias_pad, lax.axis_index('x') * SLICE, SLICE, ZERO)
        bias_cols = jnp.broadcast_to(bias_mine[:, np.newaxis], (SLICE, LANES)).reshape(-1, PIECE, LANES)
        partial = head_lse(final_bf, w_t, bias_row)
        stats = head_lse(final_bf, w_t, bias_row, partial)
        *gathered, count, log_norm = head_gw(stats, [packet, *from_sides, *across], w_t, bias_cols)
        scale = 1.0 / count[0, :1]

        last = [ORDERS[order][-1] for *_, order, _ in PARTS]
        ways = [way for *_, way in PARTS]
        from_left = [hop(g, a, RIGHT) for g, a in zip(gathered, last)]
        from_right = [hop(g, a, LEFT) for g, a in zip(gathered, last)]
        far = [hop((from_left, from_right)[way][n], a, (RIGHT, LEFT)[way]) for n, (way, a) in enumerate(zip(ways, last))]

        final_bf, _ = lax.optimization_barrier((final_bf, count))
        own_mask = mask_f[0][:, np.newaxis] > ZERO
        own_tag = labels[0][:, np.newaxis] - tp * vocab
        wide = lambda column: jnp.broadcast_to(column, (tokens, LANES))
        lse_b = wide(jnp.where(own_mask, log_norm.reshape(tokens, ONE), -NEG))
        tag_b = wide(jnp.where(own_mask & (own_tag < vocab), own_tag, -ONE))
        grad_final, target, grad_b_head = head_gz(final_bf, w_t, bias_row, lse_b, tag_b)
        hits = jnp.sum(target).reshape(ONE, ONE)
        loss_part = jnp.sum(mask_f * log_norm) - (hits + swap(hits))
        grad_final = grad_final + swap(grad_final)

        grad_resid, grad_lnf_gain, grad_lnf_bias = norm_backward(grad_final, fin_hat, fin_inv, lnf_gain)
        grad_b_fc_out = jnp.sum(grad_resid, axis=ZERO)
        grad_block = grad_resid.astype(BF16)
        grad_context = dot(grad_block, wo, NT).astype(BF16)
        grad_q, grad_k, grad_v = attn_bwd(qs, k_rot, v_proj, grad_context, lse_att, *tables, score_scale)
        grad_pre, = gelu_vjp(dot(grad_block, w_fc_out, NT))
        grad_b_fc_in = jnp.sum(grad_pre, axis=ZERO)
        grad_pre = grad_pre.astype(BF16)
        grad_normed = dot(grad_q, wq, NN) + dot(grad_k, wk, NN) + dot(grad_v, wv, NN) + dot(grad_pre, w_fc_in, NT)
        grad_normed = grad_normed + swap(grad_normed)
        grad_ln_in, grad_ln_gain, grad_ln_bias = norm_backward(grad_normed, ln_hat, ln_inv, ln_gain)
        grad_hidden = ((grad_resid + grad_ln_in) * scale).astype(BF16)

        vectors = [grad_ln_gain, grad_ln_bias, grad_b_fc_in, grad_b_fc_out, grad_lnf_gain, grad_lnf_bias,
                   jnp.broadcast_to(loss_part[0], (dim,)), jnp.sum(grad_b_head, axis=ZERO)]
        ends = list(np.cumsum([v.shape[0] for v in vectors]))
        vectors.append(jnp.zeros((BLOCK[1][0] * RING ** 3 * dim - int(ends[-1]),), F32))
        cube = lambda value, n: value.reshape(-1, RING, RING, BLOCK[n][0], dim)
        first = [cube(dot(g, h, TN), 0) for g, h in ((grad_q, normed), (grad_k, normed), (grad_v, normed), (context, grad_block))]
        sums = chip_sum((first, [cube(jnp.concatenate(vectors), 1)], [cube(dot(gelu_bf, grad_block, TN), 2)],
                         [cube(dot(normed, grad_pre[:, cols], TN), 3) for cols in chunks(grad_pre.shape[-1], dim)]))
        weights, small, fc_out, fc_in = (s.reshape(-1, dim) * scale for s in sums)
        pieces = [small.reshape(-1)[end - v.shape[0]:end] for v, end in zip(vectors, ends)]
        back = lambda n: jnp.moveaxis(weights[n * lanes:(n + ONE) * lanes].reshape(heads, head_dim, dim), -ONE, ZERO)

        coords = jnp.stack([lax.axis_index(a) for a in DP]).astype(jnp.int32)
        grad_w_head = place([(0, dict(enumerate(gathered)))], scale, coords, vocab)
        grad_w_head = place([(3, dict(enumerate(from_left))), (1, dict(enumerate(from_right)))], scale, coords, vocab, grad_w_head)
        grad_w_head = place([(2, dict(enumerate(far)))], scale, coords, vocab, grad_w_head)
        gains = pieces[:2], pieces[2], pieces[3:6]
        return (pieces[6][0], grad_hidden[np.newaxis], *gains[0], back(0), back(1), back(2),
                weights[3 * lanes:].reshape(heads, head_dim, dim), jnp.concatenate([fc_in[:dim], fc_in[dim:]], axis=ONE),
                gains[1], fc_out, *gains[2], grad_w_head.T, pieces[7][:vocab])

    return jax.shard_map(local_step, mesh=mesh, in_specs=DATA_SPECS + PARAM_SPECS,
                         out_specs=(P(), P(DP, None, None)) + PARAM_SPECS, check_vma=False)
```

```python
import functools
import itertools
import jax
import jax.numpy as jnp
import numpy as np
from jax import lax
from jax.experimental import pallas as pl
from jax.experimental.pallas import tpu as pltpu
from jax.sharding import Mesh, PartitionSpec as P

F32, BF16 = jnp.float32, jnp.bfloat16
NT = (((1,), (1,)), ((), ()))
NN = (((1,), (0,)), ((), ()))
TN = (((0,), (0,)), ((), ()))
NEG = -1e30
LN_EPS = 1e-5
ROPE_BASE = 10000.0
LANES, SUBLANES = 128, 8
MICROSECOND = 1_000_000_000
ZERO, ONE, TWO, RING = 0, 1, 2, 4
DP = ('z', 'y', 'x')
DATA_SPECS = (P(DP, None, None), P(DP, None), P(DP, None))
PARAM_SPECS = (P(None), P(None), P(None, 'tp', None), P(None, 'tp', None), P(None, 'tp', None),
               P('tp', None, None), P(None, 'tp'), P('tp'), P('tp', None), P(None), P(None), P(None),
               P(None, 'tp'), P('tp'))
TURNS = (1, 3)
RIGHT, LEFT, _ = ([(i, (i + turn) % RING) for i in range(RING)] for turn in (*TURNS, TWO))
SWAP = [(0, 1), (1, 0)]
UNIT = 200
PIECE = RING * UNIT
HALF_SLICE = RING * PIECE
SLICE = TWO * HALF_SLICE
ORDERS = (('x', 'y', 'z'), ('y', 'z', 'x'), ('z', 'x', 'y'))
PARTS = ((72, 0, 0, 0, 0), (64, 72, 0, 0, 1), (64, 136, 0, 1, 0), (64, 0, 1, 1, 1), (64, 64, 1, 2, 0), (72, 128, 1, 2, 1))
BLOCK = (0, 1, 2, 0, 1, 2)
ROWS = 8
FEW = 16
HALVES = (pl.ds(0, 2), pl.ds(2, 2))
MESH_ID = pl.DeviceIdType.MESH
ANY, WHOLE, SCALARS = (pl.BlockSpec(memory_space=space) for space in (pl.ANY, pltpu.VMEM, pltpu.SMEM))


def dot(a, b, dims):
    return lax.dot_general(a, b, dims, preferred_element_type=F32)


def iota(shape, axis, dtype=jnp.int32):
    return lax.broadcasted_iota(dtype, shape, axis)


def params(collective=None):
    return pltpu.CompilerParams(vmem_limit_bytes=60 * 2 ** 20, collective_id=collective, has_side_effects=collective is not None)


def cost(us, transfer=1):
    return pl.CostEstimate(flops=us * MICROSECOND, bytes_accessed=transfer, transcendentals=1)


def struct(shape, dtype=F32):
    return jax.ShapeDtypeStruct(shape, dtype)


def origin(*_):
    return (0, 0)


def row_block(i, *_):
    return (i, 0)


def column_block(i, *_):
    return (0, i)


def chunks(total, size=LANES):
    return [slice(at, at + size) for at in range(ZERO, total, size)]


def as_row(column):
    return jnp.transpose(jnp.broadcast_to(column, (column.shape[0], LANES)))[0:1]


def head_lse(z, w_t, bias, begin=None, tile=2560, sub=512):
    tokens, dim = z.shape
    vocab = w_t.shape[0]
    steps = pl.cdiv(vocab, tile)
    early = steps * 3 // 5
    offset = ZERO if begin is None else early

    def kernel(z_ref, w_ref, b_ref, *refs):
        step = pl.program_id(ZERO) + offset
        *begins, m_ref, s_ref = refs
        out_ref = begins.pop() if begins else None

        @pl.when(step == offset)
        def _():
            m_ref[...] = begins[0][...] if begins else jnp.full_like(m_ref, NEG)
            s_ref[...] = begins[1][...] if begins else jnp.zeros_like(s_ref)

        def work(last):
            zz = z_ref[...]
            for part in chunks(tile, sub):
                l = dot(zz, w_ref[part, :], NT) + b_ref[:, part]
                if last:
                    l = jnp.where(iota(l.shape, ONE) < vocab - step * tile - part.start, l, NEG)
                lanes = [l[:, c] for c in chunks(sub)]
                m_old = m_ref[...]
                m_new = jnp.maximum(m_old, functools.reduce(jnp.maximum, lanes))
                s_ref[...] = s_ref[...] * jnp.exp(m_old - m_new) + sum(jnp.exp(x - m_new) for x in lanes)
                m_ref[...] = m_new

        pl.when(step < steps - ONE)(lambda: work(last=False))

        @pl.when(step == steps - ONE)
        def _():
            if out_ref is None:
                return
            work(last=True)
            top = jnp.max(m_ref[...], axis=ONE, keepdims=True)
            total = jnp.sum(s_ref[...] * jnp.exp(m_ref[...] - top), axis=ONE, keepdims=True)
            out_ref[0:1] = as_row(top)
            out_ref[1:2] = as_row(total)

    state = pl.BlockSpec((tokens, LANES), origin)
    first = begin is None
    return pl.pallas_call(
        kernel, grid=(early if first else steps - early,),
        in_specs=[pl.BlockSpec((tokens, dim), origin), pl.BlockSpec((tile, dim), lambda i: (i + offset, ZERO)),
                  pl.BlockSpec((ONE, tile), lambda i: (ZERO, i + offset))] + ([] if first else [state] * TWO),
        out_specs=[state] * TWO if first else pl.BlockSpec((TWO, tokens), origin),
        out_shape=[struct((tokens, LANES))] * TWO if first else struct((TWO, tokens)),
        scratch_shapes=[] if first else [pltpu.VMEM((tokens, LANES), F32)] * TWO,
        compiler_params=params(), cost_estimate=cost(19), name='head_lse_first' if first else 'head_lse_rest',
    )(z, w_t, bias, *(begin or ()))


def swap_pairs(x, even):
    return jnp.where(even, pltpu.roll(x, LANES - ONE, ONE), pltpu.roll(x, ONE, ONE))


def halves_of(value, low):
    empty = jnp.zeros_like(value)
    return jnp.where(low, value, empty), jnp.where(low, empty, value)


def attn_fwd(u, wq, wk, wv, cos_t, sin_t, scale, blk=256):
    tokens, dim = u.shape
    lanes = wq.shape[0]

    def kernel(u_ref, wq_ref, wk_ref, wv_ref, c_ref, s_ref, qs_ref, k_ref, v_ref, ctx_ref, lse_ref):
        uu, cc, ss = u_ref[...], c_ref[...], s_ref[...]
        even = iota((tokens, LANES), ONE) % TWO == ZERO
        q = dot(uu, wq_ref[...], NT)
        qs_ref[...] = ((q * cc + swap_pairs(q, even) * ss).astype(BF16).astype(F32) * scale).astype(BF16)
        k = dot(uu, wk_ref[...], NT)
        k_ref[...] = (k * cc + swap_pairs(k, even) * ss).astype(BF16)
        v_ref[...] = dot(uu, wv_ref[...], NT).astype(BF16)
        low = iota((blk, LANES), ONE) < LANES // TWO
        causal = iota((blk, blk), ONE) <= iota((blk, blk), ZERO)
        for rows in chunks(tokens, blk):
            before, keys = slice(rows.start), slice(rows.stop)
            out = []
            for h, qh in enumerate(halves_of(qs_ref[rows, :], low)):
                s = jnp.where(causal, dot(qh, k_ref[rows, :], NT), NEG)
                if rows.start:
                    s = jnp.concatenate([dot(qh, k_ref[before, :], NT), s], axis=ONE)
                m = jnp.max(s, axis=ONE, keepdims=True)
                e = jnp.exp(s - m)
                l = jnp.sum(e, axis=ONE, keepdims=True)
                out.append(dot((e * (1.0 / l)).astype(BF16), v_ref[keys, :], NN))
                lse_ref[ZERO, h:h + ONE, rows] = as_row(m + jnp.log(l))
            ctx_ref[rows, :] = jnp.where(low, *out).astype(BF16)

    pair, wide = pl.BlockSpec((tokens, LANES), column_block), pl.BlockSpec((tokens, LANES), origin)
    return pl.pallas_call(
        kernel, grid=(lanes // LANES,),
        in_specs=[pl.BlockSpec((tokens, dim), origin)] + [pl.BlockSpec((LANES, dim), row_block)] * 3 + [wide] * TWO,
        out_specs=[pair] * RING + [pl.BlockSpec((ONE, TWO, tokens), lambda g: (g, ZERO, ZERO))],
        out_shape=[struct((tokens, lanes), BF16)] * RING + [struct((lanes // LANES, TWO, tokens))],
        compiler_params=params(), cost_estimate=cost(13), name='attn_fwd',
    )(u, wq, wk, wv, cos_t, sin_t)


def attn_bwd(qs, k, v, dctx, lse, cos_t, sin_t, scale, blk=256):
    tokens, lanes = qs.shape

    def kernel(qs_ref, k_ref, v_ref, do_ref, lse_ref, c_ref, s_ref, dq_ref, dk_ref, dv_ref, dka_ref, dva_ref):
        low = iota((blk, LANES), ONE) < LANES // TWO
        causal = iota((blk, blk), ZERO) <= iota((blk, blk), ONE)
        even = iota((blk, LANES), ONE) % TWO == ZERO

        def unrotate(x, rows):
            return (x * c_ref[rows, :] - swap_pairs(x, even) * s_ref[rows, :]).astype(BF16)

        dka_ref[...] = jnp.zeros_like(dka_ref)
        dva_ref[...] = jnp.zeros_like(dva_ref)
        for rows in chunks(tokens, blk):
            before, keys = slice(rows.start), slice(rows.stop)
            dqs = []
            for h, (qh, doh) in enumerate(zip(halves_of(qs_ref[rows, :], low), halves_of(do_ref[rows, :], low))):
                norm = lse_ref[ZERO, h:h + ONE, rows]
                p = jnp.where(causal, jnp.exp(dot(k_ref[rows, :], qh, NT) - norm), 0.0)
                if rows.start:
                    p = jnp.concatenate([jnp.exp(dot(k_ref[before, :], qh, NT) - norm), p], axis=ZERO)
                dp = dot(v_ref[keys, :], doh, NT)
                ds = (p * (dp - jnp.sum(p * dp, axis=ZERO, keepdims=True))).astype(BF16)
                dva_ref[keys, :] += dot(p.astype(BF16), doh, NN)
                dka_ref[keys, :] += dot(ds, qh, NN)
                dqs.append(dot(ds, k_ref[keys, :], TN))
            dq_ref[rows, :] = unrotate(jnp.where(low, *dqs) * scale, rows)
        for rows in chunks(tokens, blk):
            dk_ref[rows, :] = unrotate(dka_ref[rows, :], rows)
            dv_ref[rows, :] = dva_ref[rows, :].astype(BF16)

    pair, wide = pl.BlockSpec((tokens, LANES), column_block), pl.BlockSpec((tokens, LANES), origin)
    return pl.pallas_call(
        kernel, grid=(lanes // LANES,),
        in_specs=[pair] * RING + [pl.BlockSpec((ONE, TWO, tokens), lambda g: (g, ZERO, ZERO))] + [wide] * TWO,
        out_specs=[pair] * 3, out_shape=[struct((tokens, lanes), BF16)] * 3,
        scratch_shapes=[pltpu.VMEM((tokens, LANES), F32)] * TWO,
        compiler_params=params(), cost_estimate=cost(13), name='attn_bwd',
    )(qs, k, v, dctx, lse, cos_t, sin_t)


class Wires:
    def __init__(self, send, recv):
        self.send, self.recv, self.all = send, recv, []

    def line(self, src, dst, axis, turn):
        n = len(self.all)

        def build():
            size = TWO if axis == 'tp' else RING
            peer = {axis: lax.rem(lax.axis_index(axis) + turn, size)}
            return pltpu.make_async_remote_copy(src(), dst(), self.send.at[n], self.recv.at[n], device_id=peer, device_id_type=MESH_ID)

        self.all.append(build)
        return build

    def finish(self):
        for build in self.all:
            build().wait_send()


def start(lines):
    for build in lines:
        build().start()


def arrive(lines):
    for build in lines:
        build().wait_recv()


def greet(peers):
    barrier = pltpu.get_barrier_semaphore()
    for peer in peers:
        where = {axis: lax.rem(lax.axis_index(axis) + turn, TWO if axis == 'tp' else RING) for axis, turn in peer}
        pl.semaphore_signal(barrier, device_id=where, device_id_type=MESH_ID)
    return lambda: pl.semaphore_wait(barrier, len(peers))


class RingSum:
    def __init__(self, wires, axis, piece, halves, near, far):
        self.piece, self.halves, self.near, self.far = piece, halves, near, far
        sent = lambda part, s, turn: piece(turn).at[part[s]]
        kept = lambda part, s: far[s].at[part[s]]
        self.first = [wires.line(functools.partial(sent, halves, s, TWO), functools.partial(lambda s: near[s], s), axis, turn)
                      for s, turn in enumerate(TURNS)]
        self.plain, self.added = ([wires.line(functools.partial(sent, part, s, turn), functools.partial(kept, part, s), axis, turn)
                                   for s, turn in enumerate(TURNS)] for part in (halves[::-1], halves))

    def relay(self, sides=range(TWO)):
        for s in sides:
            arrive([self.first[s]])
            part = self.piece(TURNS[s]).at[self.halves[s]]
            part[...] = part[...] + self.near[s][...]
            start([self.added[s]])

    def result(self):
        arrive(self.plain + self.added)
        return self.piece(ZERO)[...] + (self.far[0][...] + self.far[1][...])


class FanSum:
    def __init__(self, wires, axis, piece, landing):
        self.piece, self.landing = piece, landing
        self.lines = [wires.line(functools.partial(piece, turn), functools.partial(lambda n: landing.at[n], turn - ONE), axis, turn)
                      for turn in range(ONE, RING)]

    def result(self):
        arrive(self.lines)
        return self.piece(ZERO)[...] + (self.landing[0] + self.landing[1] + self.landing[2])


class FanAll:
    def __init__(self, wires, axis, value, landing):
        self.value, self.landing, mine = value, landing, lax.axis_index(axis)
        self.lines = [wires.line(lambda: value, lambda: landing.at[mine], axis, turn) for turn in range(ONE, RING)]
        self.mine = mine

    def result(self):
        self.landing[self.mine] = self.value[...]
        arrive(self.lines)
        return self.landing[0] + self.landing[1] + (self.landing[2] + self.landing[3])


class RingGather:
    def __init__(self, wires, axis, place, relays):
        here = functools.partial(place, ZERO)
        self.step = [wires.line(here, here, axis, turn) for turn in TURNS]
        self.came, self.relays = [], []
        for way, part in relays:
            passed = functools.partial(lambda way, part: place(TURNS[ONE - way]).at[part], way, part)
            self.relays.append((way, wires.line(passed, passed, axis, TURNS[way])))
        self.idle = [s for s in range(TWO) if s not in dict(relays)]

    def relay(self):
        for way, line in self.relays:
            arrive([self.step[way]])
            start([line])

    def result(self):
        arrive([self.step[s] for s in self.idle] + [line for _, line in self.relays])


class FanGather:
    def __init__(self, wires, axis, place):
        here = functools.partial(place, ZERO)
        self.step = [wires.line(here, here, axis, turn) for turn in range(ONE, RING)]

    def result(self):
        arrive(self.step)


def coordinates():
    at = {axis: lax.axis_index(axis) for axis in DP}
    return at, lambda axis, turn: lax.rem(at[axis] + turn, RING)


def head_grads(stats, packets, w_t, bias_cols, bias_row, tile=1280):
    tokens = stats.shape[1]
    dim = w_t.shape[1]
    vocab = w_t.shape[0]
    tiles = bias_row.shape[1] // tile
    half = tokens // TWO
    block = PIECE // TWO
    low = 104
    halves = (pl.ds(ZERO, low), pl.ds(low, UNIT - low))
    colors = (('y', 'z'), ('z', 'y'))
    group = [(x, c) for c in range(TWO) for x in range(RING)][1:]
    firsts = [ZERO] * RING + [packets[3].shape[0]]
    n_packets, n_parts = len(packets), len(PARTS)

    def spot(ref, n):
        return ref.at[min(n, 3), pl.ds(firsts[n], packets[n].shape[0])]

    def kernel(stats_ref, *refs):
        packet_refs, (w_ref, cols_ref, bias_ref), refs = refs[:n_packets], refs[n_packets:n_packets + 3], refs[n_packets + 3:]
        outs, (count_out, norm_out, gz_ref, t_ref, gb_ref), refs = refs[:n_parts], refs[n_parts:n_parts + 5], refs[n_parts + 5:]
        (acc, w_bufs, col_bufs, zb, own, theirs, heard, norms, tags, shard, tally, big_w, lse_cols, tag_cols, *lanes, send, recv, local) = refs
        at, beside = coordinates()
        tp = lax.axis_index('tp')
        wires = Wires(send, recv)

        def part_of(h):
            stage, c, s = lax.div(h, RING), lax.rem(lax.div(h, TWO), TWO), lax.rem(h, TWO)
            inner = lax.div(stage * (3 - stage), TWO)
            flip = lax.div(stage * (TWO - stage) * (3 - stage), TWO)
            ahead = inner * (1 + TWO * s) + TWO * lax.div(3 - stage, 3)
            return c * RING + lax.rem(at['y'] + (at['z'] - at['y']) * c + ahead, RING), s + flip * (1 - TWO * s)

        def fetch(h, act):
            p, side = part_of(h)
            slot = lax.rem(h, TWO)
            row = pl.multiple_of(at['x'] * SLICE + p * PIECE + side * block, 16)
            whole = row + block <= vocab

            def move(size):
                act(pltpu.make_async_copy(w_ref.at[pl.ds(row, size)], w_bufs.at[slot, pl.ds(ZERO, size)], local.at[slot]))

            pl.when(whole)(functools.partial(move, block))
            pl.when(jnp.logical_and(row < vocab, jnp.logical_not(whole)))(functools.partial(move, vocab % block))
            act(pltpu.make_async_copy(cols_ref.at[p * TWO + side], col_bufs.at[slot], local.at[TWO + slot]))
            return p, side, slot, row

        def begin(copy):
            copy.start()

        def end(copy):
            copy.wait()

        entered = greet([(('x', x), ('tp', c)) for x, c in group] + [((a, t),) for a in ('y', 'z') for t in range(ONE, RING)])
        fetch(ZERO, begin)
        loads = [pltpu.make_async_copy(ref, spot(own, n), local.at[RING + n]) for n, ref in enumerate(packet_refs)]
        for load in loads:
            load.start()
        entered()
        news = []
        for n, (x, c) in enumerate(group):
            where = {'x': beside('x', x), 'tp': lax.rem(tp + c, TWO)}
            news.append(pltpu.make_async_remote_copy(stats_ref, heard.at[n + ONE], send.at[n], recv.at[n], device_id=where, device_id_type=MESH_ID))
            wires.all.append(functools.partial(lambda n: news[n], n))
            news[n].start()
        swaps = [wires.line(functools.partial(lambda n: packet_refs[n], n), functools.partial(spot, theirs, n), 'tp', ONE)
                 for n in range(n_packets)]
        start(swaps)
        mine = pl.multiple_of(tp * half, half)
        other = pl.multiple_of(half - tp * half, half)
        for load in loads:
            load.wait()
        for r in range(RING):
            zb[r, pl.ds(mine, half), :] = own[r, ZERO:half].astype(BF16)
        for copy in news:
            copy.wait_recv()
        heard[0] = stats_ref[...]
        for r, turn in enumerate((0, 1, 3, 2)):
            a, b = heard[turn], heard[turn + RING]
            top = jnp.maximum(a[0:1], b[0:1])
            norm = top + jnp.log(a[1:2] * jnp.exp(a[0:1] - top) + b[1:2] * jnp.exp(b[0:1] - top))
            label, mask = (jnp.concatenate([own[r, half + n:half + n + ONE] for n in (row, row + ONE)], axis=ONE) for row in (ZERO, TWO))
            tag = label - (tp * vocab).astype(F32)
            norms[r] = jnp.where(mask > 0.0, norm, -NEG)
            tags[r] = jnp.where((mask > 0.0) & (tag < vocab), tag, NEG)
            seen = jnp.broadcast_to(jnp.sum(mask, axis=ONE, keepdims=True), tally.shape[1:])
            tally[6] = seen if r == ZERO else tally[6] + seen
            if r == ZERO:
                norm_out[...] = norm
        lse_cols[...] = jnp.transpose(jnp.broadcast_to(norms[0], (LANES, tokens)))
        tag_cols[...] = jnp.transpose(jnp.broadcast_to(tags[0], (LANES, tokens)))
        arrive(swaps)
        for r in range(RING):
            zb[r, pl.ds(other, half), :] = theirs[r, ZERO:half].astype(BF16)

        pieces = [functools.partial(lambda c, axis, turn: acc.at[c * RING + beside(axis, turn)], c, axis) for c, (axis, _) in enumerate(colors)]
        sums = [RingSum(wires, colors[c][0], pieces[c], HALVES, [lanes[0].at[c], lanes[1].at[c]], [lanes[2].at[c], lanes[3].at[c]])
                for c in range(TWO)]
        votes = FanSum(wires, 'y', lambda turn: tally.at[6], tally.at[pl.ds(0, 3)])

        def unit(h, carry):
            p, side, slot, first_row = fetch(h, end)

            @pl.when(h + ONE < RING * RING)
            def _():
                fetch(h + ONE, begin)

            w, bias = w_bufs[slot], col_bufs[slot]
            row = (iota((block, LANES), ZERO) + first_row).astype(F32)
            logits = dot(w, zb[0], NT)
            out = []
            for r in range(RING):
                zr, norm, tag, l = zb[r], norms[r], tags[r], logits
                if r + ONE < RING:
                    logits = dot(w, zb[r + ONE], NT)
                grads = []
                for part in chunks(tokens):
                    prob = jnp.exp(l[:, part] + bias - norm[:, part])
                    grads.append((prob - jnp.where(row == tag[:, part], 1.0, 0.0)).astype(BF16))
                out.append(dot(jnp.concatenate(grads, axis=ONE), zr, NN))
            acc[p, pl.ds(side * TWO, TWO)] = sum(out).reshape(TWO, UNIT, dim)

            for c, total in enumerate(sums):
                for s in range(TWO):
                    here = TWO * c + s
                    pl.when(h == here)(functools.partial(start, total.first[s:s + ONE]))
                    pl.when(h == here + RING)(functools.partial(start, total.plain[s:s + ONE]))
                    pl.when(h == here + TWO * RING)(functools.partial(total.relay, (s,)))
            return carry

        start(votes.lines)
        lax.fori_loop(ZERO, RING * RING, unit, ZERO)

        last = (tiles - ONE) * tile

        def fetch_tile(i, act):
            slot = lax.rem(i, TWO)

            def move(size):
                act(pltpu.make_async_copy(w_ref.at[pl.ds(pl.multiple_of(i * tile, tile), size)], big_w.at[slot, pl.ds(ZERO, size)], local.at[slot]))

            pl.when(i < tiles - ONE)(functools.partial(move, tile))
            pl.when(i == tiles - ONE)(functools.partial(move, vocab - last))
            return slot

        seconds = []
        for c, (axis, side) in enumerate(colors):
            kept = c * RING + at[axis]
            seconds.append(RingSum(wires, side, functools.partial(lambda kept, side, turn: acc.at[kept, beside(side, turn)], kept, side),
                                   halves, [lanes[4].at[c], lanes[5].at[c]], [lanes[6].at[c], lanes[7].at[c]]))
        more_votes = FanSum(wires, 'z', lambda turn: tally.at[7], tally.at[pl.ds(3, 3)])
        keep, steps, nexts = [], [], []
        for n, (rows, offset, c, order, way) in enumerate(PARTS):
            a1, a2, _ = ORDERS[order]
            home = functools.partial(lambda n, a1, a2, turn: outs[n].at[at[a2], beside(a1, turn)], n, a1, a2)
            keep.append(functools.partial(lambda n, c, offset, rows, home: pltpu.make_async_copy(
                shard.at[c, pl.ds(offset, rows)], home(ZERO), local.at[RING + n_packets + n]), n, c, offset, rows, home))
            steps.append(RingGather(wires, a1, home, [(way, pl.ds(ZERO, rows))]))
            nexts.append(RingGather(wires, a2, functools.partial(lambda n, a2, turn: outs[n].at[beside(a2, turn)], n, a2), [(way, pl.ds(ZERO, RING))]))

        def first_sums():
            tally[7] = votes.result()
            start(more_votes.lines)
            for c, (axis, _) in enumerate(colors):
                acc[c * RING + at[axis]] = sums[c].result()
                start(seconds[c].first + seconds[c].plain)

        def second_sums():
            for c, total in enumerate(seconds):
                shard[c] = total.result()
            count_out[...] = more_votes.result()
            for copy in keep:
                copy().start()
            for copy in keep:
                copy().wait()
            for gather in steps:
                start(gather.step)

        def second_axis():
            for gather, onward in zip(steps, nexts):
                gather.result()
                start(onward.step)

        def relays(group):
            for one in group:
                one.relay()

        events = {2: first_sums, 4: lambda: relays(seconds), 7: second_sums, 9: lambda: relays(steps), 11: second_axis, 18: lambda: relays(nexts)}

        def gz_tile(i, carry):
            slot = fetch_tile(i, end)

            @pl.when(i + ONE < tiles)
            def _():
                fetch_tile(i + ONE, begin)

            w = big_w[slot]
            l = dot(zb[0], w, NT) + bias_ref[i]
            norm, rel = lse_cols[...], tag_cols[...] - (i * tile).astype(F32)
            lane = iota((tokens, LANES), ONE).astype(F32)
            grads, targets = [], []
            for c in chunks(tile):
                hit = lane == rel - c.start
                grads.append(jnp.exp(l[:, c] - norm) - jnp.where(hit, 1.0, 0.0))
                targets.append(jnp.where(hit, l[:, c], 0.0))
            t_ref[...] += sum(targets)
            grad = jnp.concatenate(grads, axis=ONE)
            gb_ref[i] = jnp.sum(grad.reshape(-1, SUBLANES, tile), axis=ZERO)
            gz_ref[...] += dot(grad.astype(BF16), w, NN)
            for when, act in events.items():
                pl.when(i + ONE == when)(act)
            return carry

        gz_ref[...] = jnp.zeros_like(gz_ref)
        t_ref[...] = jnp.zeros_like(t_ref)
        fetch_tile(ZERO, begin)
        lax.fori_loop(ZERO, tiles, gz_tile, ZERO)
        for gather in nexts:
            gather.result()
        wires.finish()

    copies = len(group) + n_packets + TWO * 3 + TWO * TWO * 6 + n_parts * TWO * 3
    row_vector = pltpu.VMEM((RING, ONE, tokens), F32)
    packet = pltpu.VMEM((RING, *packets[0].shape), F32)
    column = pltpu.VMEM((tokens, LANES), F32)
    lane = lambda *shape: [pltpu.VMEM((TWO, *shape, dim), F32)]
    return pl.pallas_call(
        kernel, in_specs=[WHOLE] + [ANY] * n_packets + [ANY, ANY, WHOLE], out_specs=[ANY] * n_parts + [WHOLE] * 5,
        out_shape=[struct((RING, RING, part[0], dim)) for part in PARTS] + [struct((SUBLANES, LANES)), struct((ONE, tokens)),
                   struct((tokens, dim)), struct((tokens, LANES)), struct((tiles, SUBLANES, tile))],
        scratch_shapes=[pltpu.VMEM((TWO * RING, RING, UNIT, dim), F32), pltpu.VMEM((TWO, block, dim), BF16), pltpu.VMEM((TWO, block, LANES), F32),
                        pltpu.VMEM((RING, tokens, dim), BF16), packet, packet, pltpu.VMEM((TWO * RING, TWO, tokens), F32),
                        row_vector, row_vector, pltpu.VMEM((TWO, UNIT, dim), F32), pltpu.VMEM((TWO * RING, SUBLANES, LANES), F32),
                        pltpu.VMEM((TWO, tile, dim), BF16), column, column,
                        *lane(TWO, UNIT) * TWO, *lane(RING, UNIT) * TWO, *lane(low), *lane(UNIT - low), *lane(UNIT) * TWO,
                        pltpu.SemaphoreType.DMA((copies,)), pltpu.SemaphoreType.DMA((copies,)),
                        pltpu.SemaphoreType.DMA((RING + n_packets + n_parts,))],
        compiler_params=params(1), cost_estimate=cost(150), name='head_grads',
    )(stats, *packets, w_t, bias_cols, bias_row.reshape(tiles, ONE, tile))


def chip_sum(inputs, small, count_tile):
    count = len(BLOCK)
    flat = [piece for group in inputs for piece in group]
    n_flat = len(flat)
    dim = small.shape[-1]
    few = small.shape[0] // RING

    def kernel(*refs):
        ins, (small_ref, tile_ref), refs = refs[:n_flat], refs[n_flat:n_flat + TWO], refs[n_flat + TWO:]
        outs, small_out, refs = refs[:count], refs[count], refs[count + ONE:]
        acc, bufs = refs[:count], [refs[count * n:count * (n + ONE)] for n in range(ONE, 7)]
        over_x, over_y, over_z, sums, send, recv, local = refs[7 * count:]
        at, beside = coordinates()
        wires = Wires(send, recv)
        scale = 1.0 / tile_ref[0:1, 0:1]
        entered = greet([((a, t),) for a in DP for t in range(ONE, RING)])
        loads, used = [[] for _ in BLOCK], ZERO
        for k, group in enumerate(inputs):
            row = ZERO
            for piece in group:
                rows = piece.shape[0]
                loads[k].append(pltpu.make_async_copy(ins[used], acc[k].at[pl.ds(row, rows)], local.at[used]))
                loads[k][-1].start()
                row, used = row + rows, used + ONE
        entered()

        def cell(ref, k, fixed, free):
            axes = ORDERS[BLOCK[k]]
            return lambda turn: ref[k].at[(*(at[a] for a in axes[:fixed]), *(beside(a, turn) for a in axes[fixed:free]))]

        little = FanSum(wires, 'x', lambda turn: small_ref.at[beside('x', turn)], over_x)
        start(little.lines)
        stages = []
        for k, order in enumerate(BLOCK):
            stages.append(RingSum(wires, ORDERS[order][0], cell(acc, k, 0, 1), HALVES, [bufs[0][k], bufs[1][k]], [bufs[2][k], bufs[3][k]]))
            for load in loads[k]:
                load.wait()
            start(stages[k].first + stages[k].plain)
        sums[0] = little.result()
        little = FanAll(wires, 'y', sums.at[0], over_y)
        start(little.lines)
        for stage in stages:
            stage.relay()
        sums[1] = little.result()
        little = FanAll(wires, 'z', sums.at[1], over_z)
        start(little.lines)
        for level in (ONE, TWO):
            for k, order in enumerate(BLOCK):
                whole = cell(acc, k, level, level)(ZERO)
                whole[...] = stages[k].result()
                stages[k] = FanSum(wires, ORDERS[order][level], cell(acc, k, level, level + ONE), bufs[3 + level][k])
                start(stages[k].lines)
        small_out[at['x']] = little.result() * scale
        little = FanGather(wires, 'x', lambda turn: small_out.at[beside('x', turn)])
        start(little.step)
        for k, order in enumerate(BLOCK):
            whole = cell(outs, k, 3, 3)(ZERO)
            whole[...] = stages[k].result() * scale
            stages[k] = FanGather(wires, ORDERS[order][TWO], cell(outs, k, 2, 3))
            start(stages[k].step)
        for k, order in enumerate(BLOCK):
            stages[k].result()
            stages[k] = FanGather(wires, ORDERS[order][ONE], cell(outs, k, 1, 2))
            start(stages[k].step)
        for k, order in enumerate(BLOCK):
            stages[k].result()
            stages[k] = RingGather(wires, ORDERS[order][0], cell(outs, k, 0, 1), list(enumerate(HALVES)))
            start(stages[k].step)
        for stage in stages:
            stage.relay()
        for stage in stages:
            stage.result()
        little.result()
        wires.finish()

    copies = count * (6 + 3 * RING + RING) + 3 * RING

    def buffers(*shape):
        return [pltpu.VMEM((*shape, ROWS, dim), F32)] * count

    landing = pltpu.VMEM((RING, few, dim), F32)
    return pl.pallas_call(
        kernel, in_specs=[ANY] * n_flat + [WHOLE] * TWO, out_specs=[WHOLE] * (count + ONE),
        out_shape=[struct((RING, RING, RING, ROWS, dim))] * count + [struct((RING, few, dim))],
        scratch_shapes=[*buffers(RING, RING, RING), *buffers(TWO, RING) * TWO, *buffers(RING, RING) * TWO, *buffers(3, RING), *buffers(3),
                        pltpu.VMEM((3, few, dim), F32), landing, landing, pltpu.VMEM((TWO, few, dim), F32),
                        pltpu.SemaphoreType.DMA((copies,)), pltpu.SemaphoreType.DMA((copies,)), pltpu.SemaphoreType.DMA((n_flat,))],
        compiler_params=params(2), cost_estimate=cost(60), name='chip_sum',
    )(*flat, small.reshape(RING, few, dim), count_tile)


def place(groups, scale, coords, vocab, into=None):
    jobs = [(shift, n, array) for shift, arrays in groups for n, array in arrays.items()]
    dim = jobs[0][-1].shape[-1]
    steps = RING * TWO
    kept = () if into is None else (into,)
    jobs_at = {(shift, n): j for j, (shift, n, _) in enumerate(jobs)}

    def kernel(coord_ref, scale_ref, *refs):
        ins, (out_ref, bufs, sems) = refs[:len(jobs)], refs[-3:]
        step = pl.program_id(ZERO)

        def each(step, act):
            slot = lax.rem(step, TWO)
            for m, (shift, n, _) in itertools.product(range(TWO), jobs):
                j = jobs_at[shift, n]
                rows, offset, c, order, _ = PARTS[n]
                a1, a2, a3 = ORDERS[order]
                at = {a1: lax.rem(step, TWO) * TWO + m, a2: lax.div(step, TWO), a3: lax.rem(coord_ref[DP.index(a3)] + shift, RING)}
                first, second = (('y', 'z'), ('z', 'y'))[c]
                row = pl.multiple_of(at['x'] * SLICE + c * HALF_SLICE + at[first] * PIECE + at[second] * UNIT + offset, SUBLANES)
                edge = vocab % UNIT - offset
                whole = row + rows <= vocab

                def move(size):
                    act(pltpu.make_async_copy(bufs.at[slot, j, m, pl.ds(ZERO, size)], out_ref.at[pl.ds(row, size)], sems.at[slot, m, j]))

                pl.when(whole)(functools.partial(move, rows))
                if ZERO < edge < rows:
                    pl.when(jnp.logical_and(row < vocab, jnp.logical_not(whole)))(functools.partial(move, edge))

        @pl.when(step >= TWO)
        def _():
            each(step - TWO, lambda copy: copy.wait())

        for j, (_, n, _) in enumerate(jobs):
            bufs[lax.rem(step, TWO), j, :, ZERO:PARTS[n][0]] = ins[j][ZERO] * scale_ref[ZERO]
        each(step, lambda copy: copy.start())

        @pl.when(step == steps - ONE)
        def _():
            each(step - ONE, lambda copy: copy.wait())
            each(step, lambda copy: copy.wait())

    blocks = [pl.BlockSpec((ONE, TWO, PARTS[n][0], dim), lambda i: (i // TWO, i % TWO, ZERO, ZERO)) for _, n, _ in jobs]
    return pl.pallas_call(
        kernel, grid=(steps,), in_specs=[SCALARS, SCALARS, *blocks] + [ANY for _ in kept], out_specs=ANY,
        out_shape=struct((vocab, dim)), input_output_aliases={TWO + len(jobs): ZERO for _ in kept},
        scratch_shapes=[pltpu.VMEM((TWO, len(jobs), TWO, 72, dim), F32), pltpu.SemaphoreType.DMA((TWO, TWO, len(jobs)))],
        compiler_params=params(), cost_estimate=cost(2 * len(jobs)),
    )(coords, scale, *[array for *_, array in jobs], *kept)


def norm_forward(terms, row, gain, shift):
    tokens, dim = terms[0].shape

    def kernel(row_ref, gain_ref, shift_ref, *refs):
        ins, (bf_ref, out_ref, hat_ref, inv_ref) = refs[:len(terms)], refs[len(terms):]
        first, *others = (ref[...].astype(F32) for ref in ins)
        values = first + sum(others[1:], others[0]) + row_ref[...] if others else first
        centered = values - jnp.mean(values, axis=-ONE, keepdims=True)
        inv = lax.rsqrt(jnp.mean(centered * centered, axis=-ONE, keepdims=True) + LN_EPS)
        hat = centered * inv
        out = hat * gain_ref[...] + shift_ref[...]
        bf_ref[...] = out.astype(BF16)
        out_ref[...] = out
        hat_ref[...] = hat
        inv_ref[...] = inv

    return pl.pallas_call(
        kernel, out_shape=[struct((tokens, dim), BF16), struct((tokens, dim)), struct((tokens, dim)), struct((tokens, ONE))],
        compiler_params=params(), cost_estimate=cost(2),
    )(*(v[np.newaxis] for v in (row, gain, shift)), *terms)


def norm_backward(grad_out, x_hat, inv_std, gain_vec):
    grad_hat = grad_out * gain_vec
    mean_grad = jnp.mean(grad_hat, axis=-ONE, keepdims=True)
    mean_proj = jnp.mean(grad_hat * x_hat, axis=-ONE, keepdims=True)
    grad_in = inv_std * (grad_hat - mean_grad - x_hat * mean_proj)
    return grad_in, jnp.sum(grad_out * x_hat, axis=ZERO), jnp.sum(grad_out, axis=ZERO)


def rope_tables(tokens, head_dim):
    rot = head_dim // 4
    inv_freq = (ROPE_BASE ** (-2.0 * np.arange(rot // TWO) / rot)).astype(np.float32)
    angles = (np.arange(tokens, dtype=np.float32)[:, np.newaxis] * inv_freq).astype(np.float64)
    cosine, sine = np.ones((tokens, head_dim), np.float32), np.zeros((tokens, head_dim), np.float32)
    cosine[:, :rot] = np.repeat(np.cos(angles), TWO, axis=ONE)
    sine[:, :rot] = np.repeat(np.sin(angles), TWO, axis=ONE) * np.tile([-1.0, 1.0], rot // TWO)
    return [np.tile(table, (ONE, LANES // head_dim)) for table in (cosine, sine)]


def hop(value, axis, way):
    return lax.ppermute(value, axis, way)


def solution(mesh):
    mesh = Mesh(mesh.devices.reshape(TWO, RING, RING, RING), ('tp', *DP))

    def local_step(hidden, labels, loss_mask, ln_gain, ln_bias, w_query, w_key, w_value, w_attn_out,
                   w_fc_in, b_fc_in, w_fc_out, b_fc_out, lnf_gain, lnf_bias, w_head, b_head):
        _, tokens, dim = hidden.shape
        _, heads, head_dim = w_query.shape
        lanes, half = heads * head_dim, tokens // TWO
        vocab = b_head.shape[0]
        score_scale = head_dim ** -0.5
        tp = lax.axis_index('tp')
        swap = lambda value: lax.ppermute(value, 'tp', SWAP)
        rows_of = lambda w: jnp.moveaxis(w, ZERO, -ONE).reshape(lanes, dim)
        wq, wk, wv = rows_of(w_query), rows_of(w_key), rows_of(w_value)
        wo = w_attn_out.reshape(lanes, dim)
        w_t = w_head.T
        tables = rope_tables(tokens, head_dim)
        mask_f = loss_mask.astype(F32)

        normed, _, ln_hat, ln_inv = norm_forward([hidden[ZERO]], ln_bias, ln_gain, ln_bias)
        qs, k_rot, v_proj, context, lse_att = attn_fwd(normed, wq, wk, wv, *tables, score_scale)
        pre_act = dot(normed, w_fc_in, NN) + b_fc_in
        gelu_out, gelu_vjp = jax.vjp(functools.partial(jax.nn.gelu, approximate=True), pre_act)
        gelu_bf = gelu_out.astype(BF16)
        block_part = dot(context, wo, NN) + dot(gelu_bf, w_fc_out, NN)
        peer_part = hop(block_part, 'tp', SWAP)
        final_bf, final_f32, fin_hat, fin_inv = norm_forward([hidden[ZERO], block_part, peer_part], b_fc_out, lnf_gain, lnf_bias)

        extra = jnp.concatenate([labels.astype(F32).reshape(TWO, half), mask_f.reshape(TWO, half), jnp.zeros((RING, half), F32)])
        packet = jnp.concatenate([lax.dynamic_slice_in_dim(final_f32, tp * half, half, ZERO), extra])
        from_sides = [hop(packet, 'x', way) for way in (RIGHT, LEFT)]
        cut = packet.shape[0] // TWO // SUBLANES * SUBLANES
        across = [hop(side, 'x', way)
                  for side, way in ((from_sides[0][:cut], RIGHT), (from_sides[1][cut:], LEFT))]

        bias_row = b_head[np.newaxis]
        bias_pad = jnp.concatenate([b_head, jnp.full((RING * SLICE - vocab,), NEG, F32)])
        bias_mine = lax.dynamic_slice_in_dim(bias_pad, lax.axis_index('x') * SLICE, SLICE, ZERO)
        bias_cols = jnp.broadcast_to(bias_mine[:, np.newaxis], (SLICE, LANES)).reshape(-1, PIECE // TWO, LANES)
        partial = head_lse(final_bf, w_t, bias_row)
        stats = head_lse(final_bf, w_t, bias_row, partial)
        *gathered, count, log_norm, grad_final, target, grad_b_head = head_grads(stats, [packet, *from_sides, *across], w_t, bias_cols, bias_pad[np.newaxis])
        scale = 1.0 / count[0, :1]

        last = [ORDERS[order][-1] for *_, order, _ in PARTS]
        ways = [way for *_, way in PARTS]
        from_left = [hop(g, a, RIGHT) for g, a in zip(gathered, last)]
        from_right = [hop(g, a, LEFT) for g, a in zip(gathered, last)]
        far = [hop((from_left, from_right)[way][n], a, (RIGHT, LEFT)[way]) for n, (way, a) in enumerate(zip(ways, last))]

        hits = jnp.sum(target).reshape(ONE, ONE)
        loss_part = jnp.sum(mask_f * log_norm) - (hits + swap(hits))
        grad_final = grad_final + swap(grad_final)

        grad_resid, grad_lnf_gain, grad_lnf_bias = norm_backward(grad_final, fin_hat, fin_inv, lnf_gain)
        grad_b_fc_out = jnp.sum(grad_resid, axis=ZERO)
        grad_block = grad_resid.astype(BF16)
        grad_context = dot(grad_block, wo, NT).astype(BF16)
        grad_q, grad_k, grad_v = attn_bwd(qs, k_rot, v_proj, grad_context, lse_att, *tables, score_scale)
        grad_pre, = gelu_vjp(dot(grad_block, w_fc_out, NT))
        grad_b_fc_in = jnp.sum(grad_pre, axis=ZERO)
        grad_pre = grad_pre.astype(BF16)
        grad_normed = dot(grad_q, wq, NN) + dot(grad_k, wk, NN) + dot(grad_v, wv, NN) + dot(grad_pre, w_fc_in, NT)
        grad_normed = grad_normed + swap(grad_normed)
        grad_ln_in, grad_ln_gain, grad_ln_bias = norm_backward(grad_normed, ln_hat, ln_inv, ln_gain)
        grad_hidden = ((grad_resid + grad_ln_in) * scale).astype(BF16)[np.newaxis]

        vectors = [grad_ln_gain, grad_ln_bias, grad_b_fc_in, grad_b_fc_out, grad_lnf_gain, grad_lnf_bias,
                   jnp.broadcast_to(loss_part[0], (dim,)), jnp.sum(grad_b_head, axis=ONE).reshape(-1)]
        ends = list(np.cumsum([v.shape[0] for v in vectors]))
        vectors.append(jnp.zeros((RING * FEW * dim - int(ends[-1]),), F32))
        rows = jnp.concatenate([v.reshape(-1, dim) for v in vectors])
        cube = lambda value: value.reshape(-1, RING, RING, ROWS, dim)
        heads_grads = [cube(dot(g, h, TN)) for g, h in ((grad_q, normed), (grad_k, normed), (grad_v, normed), (context, grad_block))]
        halves = chunks(grad_pre.shape[-1], dim)
        outer = [[cube(dot(gelu_bf[:, cols], grad_block, TN))] for cols in halves]
        inner = [[cube(dot(normed, grad_pre[:, cols], TN))] for cols in halves]
        *sums, small = chip_sum([heads_grads[:TWO], outer[0], inner[0], heads_grads[TWO:], outer[1], inner[1]], rows, count)
        sums = [s.reshape(-1, dim) for s in sums]
        pieces = [small.reshape(-1)[end - v.shape[0]:end] for v, end in zip(vectors, ends)]
        weights = [sums[n // TWO * 3][n % TWO * lanes:(n % TWO + ONE) * lanes].reshape(heads, head_dim, dim) for n in range(RING)]
        weights[:3] = [jnp.moveaxis(w, -ONE, ZERO) for w in weights[:3]]
        loss, grad_b_head = pieces[6][0], pieces[7][:vocab]
        fc_in, fc_out = jnp.concatenate([sums[2], sums[5]], axis=ONE), jnp.concatenate([sums[1], sums[4]])

        coords = jnp.stack([lax.axis_index(a) for a in DP]).astype(jnp.int32)
        grad_w_head = place([(0, dict(enumerate(gathered)))], scale, coords, vocab)
        grad_w_head = place([(3, dict(enumerate(from_left))), (1, dict(enumerate(from_right)))], scale, coords, vocab, grad_w_head)
        grad_w_head = place([(2, dict(enumerate(far)))], scale, coords, vocab, grad_w_head)
        return (loss, grad_hidden, *pieces[:2], *weights, fc_in, pieces[2], fc_out, *pieces[3:6], grad_w_head.T, grad_b_head)

    return jax.shard_map(local_step, mesh=mesh, in_specs=DATA_SPECS + PARAM_SPECS,
                         out_specs=(P(), P(DP, None, None)) + PARAM_SPECS, check_vma=False)
```
